32 devices in a mesh: dp: 4 (over z), shard: 8 (over y, x, core).
Axes of the slice: x: 2, y: 2, z: 4, core: 2. Of those that a mesh axis runs over, the one named last changes fastest.
Arguments:
- gradients: bfloat16 [4, 2, 512, 16, 512], P('dp', None, 'shard'), may hold values from -6 to 6
- owner_list: int32 [32], replicated, may hold values from 0 to 31, as said below
- row_offset: int32 [32], replicated, may hold values from 0 to 512, as said below
- col_offset: int32 [32], replicated, may hold values from 0 to 7680, as said below
- left_factor: float32 [64, 512, 512], P(('dp', 'shard')), may hold values from -32 to 32, as said below
- right_factor: float32 [64, 512, 512], P(('dp', 'shard')), may hold values from -32 to 32, as said below
- left_root: float32 [64, 512, 512], P(('dp', 'shard')), may hold values from -2 to 2, as said below
- right_root: float32 [64, 512, 512], P(('dp', 'shard')), may hold values from -2 to 2, as said below
Outputs:
- update: bfloat16 [2, 512, 16, 512], P(None, 'shard', None, 'dp')
- new_left_factor: float32 [64, 512, 512], P(('dp', 'shard'))
- new_right_factor: float32 [64, 512, 512], P(('dp', 'shard'))
- new_left_root: float32 [64, 512, 512], P(('dp', 'shard'))
- new_right_root: float32 [64, 512, 512], P(('dp', 'shard'))
The draws below stay inside these ranges and needn't reach their ends.
Inputs may be any that keep to these rules, and one draw needn't show every extreme that they name: `owner_list`: no owner is named by more than 2 entries, and some owner by exactly 2. `row_offset`: multiples of 512; with col_offset, every block of the 2 x 16 grid is named exactly once. `col_offset`: multiples of 512; with row_offset, every block of the grid is named exactly once. `left_factor`: each slot symmetric positive definite. `right_factor`: each slot symmetric positive definite. `left_root`: each slot symmetric. `right_root`: each slot symmetric.
All inputs are finite; a program needn't handle non-finite values.
Results may differ from the reference program's by a relative error of at most 0.012.
Values may be sent and summed in bfloat16 or wider, within the bound.
A program may use at most 128 MiB of HBM per device.

```python
import jax
import jax.numpy as jnp
from jax import lax

BLOCK = 512
SLOTS = 2
REPLICAS = 4
BC = 16
BR = 2
BLOCKS = 32
SLOTS_ALL = 64


def draw_owner_list(key, part):
    base = jax.random.fold_in(key, 7)
    first_key, second_key, third_key = jax.random.split(base, 3)
    owner_count = SLOTS_ALL // SLOTS
    starred = jax.random.randint(first_key, (), 0, owner_count)
    others = jax.random.permutation(second_key, SLOTS_ALL - SLOTS).astype(jnp.int32)
    others = others + SLOTS * (others >= SLOTS * starred).astype(jnp.int32)
    rest = others[:BLOCKS - SLOTS] // SLOTS
    owners = jnp.concatenate([jnp.full((SLOTS,), starred, jnp.int32), rest.astype(jnp.int32)])
    shuffle = jax.random.permutation(third_key, BLOCKS)
    return owners[shuffle].astype(jnp.int32)


def grid_order(key):
    return jax.random.permutation(jax.random.fold_in(key, 11), BLOCKS).astype(jnp.int32)


def draw_row_offset(key, part):
    return (grid_order(key) // BC * BLOCK).astype(jnp.int32)


def draw_col_offset(key, part):
    return (grid_order(key) % BC * BLOCK).astype(jnp.int32)


def factor_draw(key):
    first_key = jax.random.fold_in(key, 0)
    noise = jax.random.normal(first_key, (SLOTS_ALL, BLOCK, BLOCK), jnp.float32)
    gram = jnp.einsum('nij,nkj->nik', noise, noise, precision=lax.Precision.HIGHEST) / BLOCK
    return gram + 0.5 * jnp.eye(BLOCK, dtype=jnp.float32)[None]


def draw_left_factor(key, part):
    return factor_draw(jax.random.fold_in(key, 3))


def draw_right_factor(key, part):
    return factor_draw(jax.random.fold_in(key, 5))


def root_draw(key):
    noise = jax.random.normal(key, (SLOTS_ALL, BLOCK, BLOCK), jnp.float32)
    symmetric = (noise + jnp.swapaxes(noise, 1, 2)) / (2.0 * BLOCK ** 0.5)
    return jnp.eye(BLOCK, dtype=jnp.float32)[None] + 0.3 * symmetric


def draw_left_root(key, part):
    return root_draw(jax.random.fold_in(key, 13))


def draw_right_root(key, part):
    return root_draw(jax.random.fold_in(key, 17))


def level_of(stream_key, shape, cuts, smallest, largest):
    loudness = 1.0
    for axis_at, shards_of in cuts:
        draws = jax.random.uniform(jax.random.fold_in(jax.random.fold_in(stream_key, 6), axis_at), (shards_of,), jnp.float32, smallest / len(cuts), largest / len(cuts))
        loudness = loudness * jnp.repeat(jnp.exp(draws), shape[axis_at] // shards_of).reshape((-1,) + (1,) * (len(shape) - 1 - axis_at))
    return loudness


def centred(own_key, shape, scale, reach, cuts=(), kind=jnp.bfloat16):
    loudness = level_of(own_key, shape, cuts, -0.22, 0.18) if cuts else 1.0
    drawn = jax.random.normal(own_key, shape, jnp.float32) * scale * loudness
    return jnp.minimum(jnp.maximum(drawn, -reach), reach).astype(kind)


def setup_inputs(seed: int = 0) -> dict:
    splits = jax.random.split(jax.random.key(seed), 9)
    gradients = centred(splits[0], (REPLICAS, BR, BLOCK, BC, BLOCK), 0.5, 6.0, ((0, 4), (2, 8)))
    owner_list = draw_owner_list(jax.random.fold_in(splits[8], 71), 0)
    row_offset = draw_row_offset(jax.random.fold_in(splits[8], 71), 0)
    col_offset = draw_col_offset(jax.random.fold_in(splits[8], 71), 0)
    left_factor = draw_left_factor(jax.random.fold_in(splits[8], 71), 0)
    right_factor = draw_right_factor(jax.random.fold_in(splits[8], 71), 0)
    left_root = draw_left_root(jax.random.fold_in(splits[8], 71), 0)
    right_root = draw_right_root(jax.random.fold_in(splits[8], 71), 0)
    return {"gradients": gradients, "owner_list": owner_list, "row_offset": row_offset, "col_offset": col_offset, "left_factor": left_factor, "right_factor": right_factor, "left_root": left_root, "right_root": right_root}


decay_rate = 0.9
highest = lax.Precision.HIGHEST


def newton_root(factor, old_root):
    identity = jnp.eye(factor.shape[0], dtype=factor.dtype)
    normed = factor * (factor.shape[0] / jnp.trace(factor))
    root_sq = jnp.dot(old_root, old_root, precision=highest)
    root_quad = jnp.dot(root_sq, root_sq, precision=highest)
    coupled = jnp.dot(root_quad, normed, precision=highest)
    newton_t = (5.0 * identity - coupled) / 4.0
    return jnp.dot(old_root, newton_t, precision=highest)


def per_block(inputs):
    g_block, left_old, right_old, left_prev, right_prev = inputs
    gram_left = jnp.dot(g_block, g_block.T, preferred_element_type=jnp.float32)
    gram_right = jnp.dot(g_block.T, g_block, preferred_element_type=jnp.float32)
    left_new = decay_rate * left_old + ((1.0 - decay_rate) / BLOCK) * gram_left
    right_new = decay_rate * right_old + ((1.0 - decay_rate) / BLOCK) * gram_right
    left_next = newton_root(left_new, left_prev)
    right_next = newton_root(right_new, right_prev)
    g_float = g_block.astype(jnp.float32)
    result = jnp.dot(jnp.dot(left_next, g_float, precision=highest), right_next, precision=highest)
    return result.astype(jnp.bfloat16), left_new, right_new, left_next, right_next


def reference(gradients, owner_list, row_offset, col_offset, left_factor, right_factor, left_root, right_root):
    summed = jnp.sum(gradients.astype(jnp.float32), axis=0).astype(jnp.bfloat16)
    block_row = (row_offset // BLOCK).astype(jnp.int32)
    block_col = (col_offset // BLOCK).astype(jnp.int32)
    entry_index = jnp.arange(BLOCKS, dtype=jnp.int32)
    same_owner = owner_list[None, :] == owner_list[:, None]
    earlier = jnp.sum(same_owner & (entry_index[None, :] < entry_index[:, None]), axis=1).astype(jnp.int32)
    slot_of = (owner_list * SLOTS + earlier).astype(jnp.int32)
    pieces = summed[block_row, :, block_col, :]
    outputs = lax.map(per_block, (pieces, left_factor[slot_of], right_factor[slot_of], left_root[slot_of], right_root[slot_of]))
    blocks_out, left_new, right_new, left_next, right_next = outputs
    update = jnp.zeros((BR, BLOCK, BC, BLOCK), jnp.bfloat16).at[block_row, :, block_col, :].set(blocks_out)
    new_left_factor = left_factor.at[slot_of].set(left_new)
    new_right_factor = right_factor.at[slot_of].set(right_new)
    new_left_root = left_root.at[slot_of].set(left_next)
    new_right_root = right_root.at[slot_of].set(right_next)
    return update, new_left_factor, new_right_factor, new_left_root, new_right_root
```

```python
import functools

import jax
import jax.numpy as jnp
from jax import lax
from jax.experimental import pallas as pl
from jax.experimental.pallas import tpu as pltpu
from jax.sharding import PartitionSpec as P

decay_rate = 0.9
MESH = pl.DeviceIdType.MESH
f32 = jnp.float32
bf16 = jnp.bfloat16


def split(x):
    hi = x.astype(bf16)
    return hi, (x - hi.astype(f32)).astype(bf16)


def mm(a, b, ca=1, cb=0):
    return lax.dot_general(a, b, (((ca,), (cb,)), ((), ())), preferred_element_type=f32)


def mm3(a, b):
    return mm(a[0], b[0]) + (mm(a[0], b[1]) + mm(a[1], b[0]))


def reduce_kernel(n, blk_ref, grad_ref, out_ref, own, from_left, from_right, acc, pieces,
                  load_sem, send_sem, left_sem, right_sem):
    me = lax.axis_index("dp")
    shard = lax.axis_index("shard")
    parts, rows, cols, width = own.shape[1:]
    loads = {}
    order = []
    for j in range(n):
        for t in (n - 1 - j, j):
            if t not in order:
                order.append(t)
    for t in order:
        for b in range(parts):
            loads[t, b] = pltpu.make_async_copy(
                grad_ref.at[0, b, :, :, pl.ds(t * width, width)], own.at[t, b], load_sem.at[t, b]
            )
            loads[t, b].start()
    barrier = pltpu.get_barrier_semaphore()

    @pl.when(me > 0)
    def _():
        pl.semaphore_signal(barrier, inc=1, device_id=(me - 1, shard), device_id_type=MESH)

    @pl.when(me < n - 1)
    def _():
        pl.semaphore_signal(barrier, inc=1, device_id=(me + 1, shard), device_id_type=MESH)

    peers = (me > 0).astype(jnp.int32) + (me < n - 1).astype(jnp.int32)
    pl.semaphore_wait(barrier, peers)

    for t in order:
        for b in range(parts):
            loads[t, b].wait()

    def hop(t, b, step):
        buffer, sem = (from_left, left_sem) if step > 0 else (from_right, right_sem)
        return pltpu.make_async_remote_copy(
            src_ref=own.at[t, b],
            dst_ref=buffer.at[t, b],
            send_sem=send_sem.at[t, b],
            recv_sem=sem.at[t, b],
            device_id=(me + step, shard),
            device_id_type=MESH,
        )

    def pass_on(t, b, step):
        inner = me > 0 if step > 0 else me < n - 1
        buffer = from_left if step > 0 else from_right

        @pl.when(inner)
        def _():
            hop(t, b, step).wait_recv()
            own[t, b] = (own[t, b].astype(f32) + buffer[t, b].astype(f32)).astype(bf16)

        hop(t, b, step).start()

    for j in range(n - 1):
        for b in range(parts):
            for t, step in ((n - 1 - j, 1), (j, -1)):
                pl.when(me < t if step > 0 else me > t)(
                    functools.partial(pass_on, t, b, step)
                )
    for b in range(parts):
        acc[b] = own[me, b].astype(f32)

        @pl.when(me > 0)
        def _():
            hop(me, b, 1).wait_recv()
            acc[b] += from_left[me, b].astype(f32)

        @pl.when(me < n - 1)
        def _():
            hop(me, b, -1).wait_recv()
            acc[b] += from_right[me, b].astype(f32)

        for c in range(cols):
            pieces[b * cols + c] = acc[b, :, c, :].astype(bf16)

    @pl.loop(0, out_ref.shape[0])
    def _(s):
        out_ref[s] = pieces[blk_ref[s]]

    for t in range(n):
        for b in range(parts):

            @pl.when(me != t)
            def _():
                hop(t, b, 1).wait_send()


def power_kernel(left_ref, right_ref, lh_ref, ll_ref, rh_ref, rl_ref):
    for x_ref, h_ref, l_ref in ((left_ref, lh_ref, ll_ref), (right_ref, rh_ref, rl_ref)):
        x = split(x_ref[0])
        square = split(mm3(x, x))
        quad = split(mm3(square, square))
        hi, lo = split(mm3(quad, x))
        h_ref[0] = hi
        l_ref[0] = lo


def root_of(factor, power, old_root):
    size = factor.shape[0]
    row = lax.broadcasted_iota(jnp.int32, factor.shape, 0)
    col = lax.broadcasted_iota(jnp.int32, factor.shape, 1)
    trace = jnp.sum(jnp.where(row == col, factor, 0.0))
    return 1.25 * old_root - mm3(power, split(factor)) * (size / (4.0 * trace))


def step_kernel(dp, sh, slots, count_ref, in_ref, lf_ref, rf_ref, lr_ref, rr_ref, lh_ref, ll_ref,
                rh_ref, rl_ref, out_ref, nlf_ref, nrf_ref, nlr_ref, nrr_ref, g_ref):
    slot = pl.program_id(0)
    live = slot < count_ref[0]
    rows, width = in_ref.shape[1:]
    size = g_ref.shape[0]
    for d in range(dp):
        for s in range(sh):
            g_ref[s * rows:(s + 1) * rows, d * width:(d + 1) * width] = in_ref[
                (d * sh + s) * slots + slot
            ]
    g = g_ref[...]
    rate = (1.0 - decay_rate) / size
    left = decay_rate * lf_ref[0] + rate * mm(g, g, 1, 1)
    right = decay_rate * rf_ref[0] + rate * mm(g, g, 0, 0)
    nlf_ref[0] = jnp.where(live, left, lf_ref[0])
    nrf_ref[0] = jnp.where(live, right, rf_ref[0])
    left_root = root_of(left, (lh_ref[0], ll_ref[0]), lr_ref[0])
    nlr_ref[0] = jnp.where(live, left_root, lr_ref[0])
    right_root = root_of(right, (rh_ref[0], rl_ref[0]), rr_ref[0])
    nrr_ref[0] = jnp.where(live, right_root, rr_ref[0])
    hi, lo = split(left_root)
    product = split(mm(hi, g) + mm(lo, g))
    g_ref[...] = mm3(product, split(right_root)).astype(bf16)
    for d in range(dp):
        for s in range(sh):
            out_ref[(d * sh + s) * slots + slot] = g_ref[
                s * rows:(s + 1) * rows, d * width:(d + 1) * width
            ]


def place_kernel(slot_ref, in_ref, out_ref, acc):
    row_blocks, _, col_blocks, _ = out_ref.shape
    for b in range(row_blocks):
        for c in range(col_blocks):
            acc[b, :, c, :] = in_ref[slot_ref[b * col_blocks + c]].astype(f32)
        out_ref[b] = acc[b].astype(bf16)


def body(
    gradients, owner_list, row_offset, col_offset, left_factor, right_factor, left_root, right_root
):
    dp = lax.axis_size("dp")
    sh = lax.axis_size("shard")
    slots, size, _ = left_factor.shape
    _, parts, rows, cols, _ = gradients.shape
    width = size // dp
    total = dp * sh * slots
    blocks = owner_list.shape[0]
    block_at = row_offset // size * cols + col_offset // size
    entry_index = jnp.arange(blocks, dtype=jnp.int32)
    same_owner = owner_list[None, :] == owner_list[:, None]
    earlier = jnp.sum(same_owner & (entry_index[None, :] < entry_index[:, None]), axis=1)
    slot_of = owner_list * slots + earlier
    slot_index = jnp.arange(total, dtype=jnp.int32)
    block_of_slot = jnp.sum(
        jnp.where(slot_of[None, :] == slot_index[:, None], block_at[None, :], 0), axis=1
    ).astype(jnp.int32)
    slot_of_block = jnp.sum(
        jnp.where(block_at[None, :] == entry_index[:, None], slot_of[None, :], 0), axis=1
    ).astype(jnp.int32)
    my_index = lax.axis_index(("dp", "shard"))
    my_count = jnp.sum((owner_list == my_index).astype(jnp.int32), keepdims=True)

    smem = pl.BlockSpec(memory_space=pltpu.SMEM)
    vmem = pl.BlockSpec(memory_space=pltpu.VMEM)
    chunk = (dp, parts, rows, cols, width)
    sems = pltpu.SemaphoreType.DMA((dp, parts))
    outgoing = pl.pallas_call(
        functools.partial(reduce_kernel, dp),
        out_shape=jax.ShapeDtypeStruct((total, rows, width), bf16),
        in_specs=[smem, pl.BlockSpec(memory_space=pl.ANY)],
        out_specs=vmem,
        scratch_shapes=[
            pltpu.VMEM(chunk, bf16),
            pltpu.VMEM(chunk, bf16),
            pltpu.VMEM(chunk, bf16),
            pltpu.VMEM(chunk[1:], f32),
            pltpu.VMEM((parts * cols, rows, width), bf16),
            sems, sems, sems, sems,
        ],
        compiler_params=pltpu.CompilerParams(
            collective_id=0, has_side_effects=True, vmem_limit_bytes=48 * 2**20
        ),
        cost_estimate=pl.CostEstimate(flops=10**9, bytes_accessed=2**22, transcendentals=0),
        name="reduce_columns",
    )(block_of_slot, gradients)
    incoming = lax.all_to_all(outgoing, ("dp", "shard"), split_axis=0, concat_axis=0, tiled=True)

    matrix = pl.BlockSpec((1, size, size), lambda i: (i, 0, 0))
    half = jax.ShapeDtypeStruct((slots, size, size), bf16)
    full = jax.ShapeDtypeStruct((slots, size, size), f32)
    powers = pl.pallas_call(
        power_kernel,
        grid=(slots,),
        out_shape=[half] * 4,
        in_specs=[matrix] * 2,
        out_specs=[matrix] * 4,
        cost_estimate=pl.CostEstimate(
            flops=36 * slots * size**3, bytes_accessed=16 * slots * size**2, transcendentals=0
        ),
        name="fifth_powers",
    )(left_root, right_root)
    whole = pl.BlockSpec((total, rows, width), lambda i: (0, 0, 0))
    outbound, *news = pl.pallas_call(
        functools.partial(step_kernel, dp, sh, slots),
        grid=(slots,),
        out_shape=[jax.ShapeDtypeStruct((total, rows, width), bf16)] + [full] * 4,
        in_specs=[smem, whole] + [matrix] * 8,
        out_specs=[whole] + [matrix] * 4,
        scratch_shapes=[pltpu.VMEM((size, size), bf16)],
        compiler_params=pltpu.CompilerParams(vmem_limit_bytes=56 * 2**20),
        name="step",
    )(my_count, incoming, left_factor, right_factor, left_root, right_root, *powers)
    returned = lax.all_to_all(outbound, ("dp", "shard"), split_axis=0, concat_axis=0, tiled=True)
    update = pl.pallas_call(
        place_kernel,
        out_shape=jax.ShapeDtypeStruct((parts, rows, cols, width), bf16),
        in_specs=[smem, vmem],
        out_specs=vmem,
        scratch_shapes=[pltpu.VMEM((parts, rows, cols, width), f32)],
        name="place",
    )(slot_of_block, returned)
    return (update, *news)


def solution(mesh):
    owned = P(("dp", "shard"), None, None)
    in_specs = (P("dp", None, "shard", None, None), P(), P(), P(), owned, owned, owned, owned)
    out_specs = (P(None, "shard", None, "dp"), owned, owned, owned, owned)
    return jax.shard_map(body, mesh=mesh, in_specs=in_specs, out_specs=out_specs, check_vma=False)
```
